32 devices in a mesh: section: 4 (over y, core), dp: 8 (over z, x).
Axes of the slice: x: 2, y: 2, z: 4, core: 2. Of those that a mesh axis runs over, the one named last changes fastest.
Arguments:
- latents: bfloat16 [16, 4, 128], P('dp'), may hold values from -6 to 6
- noise: bfloat16 [16, 4, 128], P('dp'), may hold values from -6 to 6
- timesteps: int32 [16], P('dp'), may hold values from 0 to 999
- cameras: int32 [16, 4], P('dp'), may hold values from 0 to 31
- embed_in: bfloat16 [4, 1024], replicated, may hold values from -3 to 3
- camera_table: bfloat16 [32, 1024], replicated, may hold values from -6 to 6
- w_mod: bfloat16 [4, 256, 3072], P('section'), may hold values from -0.375 to 0.375
- w_qkv: bfloat16 [4, 1024, 3072], P('section'), may hold values from -0.1875 to 0.1875
- w_out: bfloat16 [4, 1024, 1024], P('section'), may hold values from -0.1875 to 0.1875
- head_out: bfloat16 [4, 1024], replicated, may hold values from -0.1875 to 0.1875
- moment_qkv: float32 [4, 1024, 3072], P('section', 'dp'), may hold values from -6 to 6
- moment_out: float32 [4, 1024, 1024], P('section', 'dp'), may hold values from -6 to 6
- second_qkv: float32 [4, 1024, 3072], P('section', 'dp'), may hold values from 0.25 to 4
- second_out: float32 [4, 1024, 1024], P('section', 'dp'), may hold values from 0.25 to 4
Outputs:
- update_qkv: float32 [4, 1024, 3072], P('section', 'dp')
- update_out: float32 [4, 1024, 1024], P('section', 'dp')
- new_moment_qkv: float32 [4, 1024, 3072], P('section', 'dp')
- new_moment_out: float32 [4, 1024, 1024], P('section', 'dp')
- new_second_qkv: float32 [4, 1024, 3072], P('section', 'dp')
- new_second_out: float32 [4, 1024, 1024], P('section', 'dp')
The draws below stay inside these ranges and needn't reach their ends.
All inputs are finite; a program needn't handle non-finite values.
Results may differ from the reference program's by a relative error of at most 0.00045.
Values may be sent and summed in bfloat16 or wider, within the bound.
A program may use at most 128 MiB of HBM per device.

```python
import math
import jax
import jax.numpy as jnp
from jax import lax

D = 1024
HEADS = 16
HEAD_DIM = 64
CH = 4
TEMB = 256
CAMERAS = 32
VIEWS = 4
SEQ = 128
SAMPLES = 16
LAYERS = 4


def set_ends(entries, own_key, least, high):
    index_at = [jax.random.randint(jax.random.fold_in(own_key, axis), (), 0, length) for axis, length in enumerate(entries.shape)]
    longest = entries.shape.index(max(entries.shape))
    next_to = index_at[:longest] + [(index_at[longest] + 1) % entries.shape[longest]] + index_at[longest + 1:]
    return entries.at[tuple(index_at)].set(least).at[tuple(next_to)].set(high)


def steps_of(stream_key, dims, cuts, least, largest):
    loudness, own = 1.0, jax.random.fold_in(stream_key, 6)
    for axis_at, blocks in cuts:
        heights = jnp.exp(jax.random.uniform(jax.random.fold_in(own, axis_at), (blocks,), jnp.float32, least / len(cuts), largest / len(cuts)))
        loudness = loudness * jnp.repeat(heights, dims[axis_at] // blocks).reshape([-1 if axis == axis_at else 1 for axis in range(len(dims))])
    return loudness


def centred(rng, dims, scale, reach, pieces=(), held_as=jnp.bfloat16):
    drawn = jax.random.normal(rng, dims, jnp.float32) * scale
    if len(pieces) > 0:
        drawn = steps_of(rng, dims, pieces, -0.22, 0.18) * drawn
    return jnp.clip(drawn, min=-reach, max=reach).astype(held_as)


def setup_inputs(seed: int = 0) -> dict:
    streams_of = jax.random.split(jax.random.key(seed), 15)
    latents = centred(streams_of[0], (SAMPLES, CH, SEQ), 1.0, 6.0, ((0, 8),))
    noise = centred(streams_of[1], (SAMPLES, CH, SEQ), 1.0, 6.0, ((0, 8),))
    timesteps = set_ends(jax.random.randint(streams_of[2], (SAMPLES,), 0, 1000), jax.random.fold_in(streams_of[2], 1), 0, 999).astype(jnp.int32)
    cameras = set_ends(jax.random.randint(streams_of[3], (SAMPLES, VIEWS), 0, CAMERAS), jax.random.fold_in(streams_of[3], 1), 0, CAMERAS - 1).astype(jnp.int32)
    embed_in = centred(streams_of[4], (CH, D), CH ** -0.5, 3.0)
    camera_table = centred(streams_of[5], (CAMERAS, D), 1.0, 6.0)
    w_mod = centred(streams_of[6], (LAYERS, TEMB, 3 * D), TEMB ** -0.5, 0.375, ((0, 4),))
    w_qkv = centred(streams_of[7], (LAYERS, D, 3 * D), D ** -0.5, 0.1875, ((0, 4),))
    w_out = centred(streams_of[8], (LAYERS, D, D), D ** -0.5, 0.1875, ((0, 4),))
    head_out = centred(streams_of[9], (CH, D), D ** -0.5, 0.1875)
    moment_qkv = centred(streams_of[10], (LAYERS, D, 3 * D), 1.0, 6.0, ((0, 4), (1, 8)), jnp.float32)
    moment_out = centred(streams_of[11], (LAYERS, D, D), 1.0, 6.0, ((0, 4), (1, 8)), jnp.float32)
    second_qkv = jnp.clip(jnp.exp(math.log(4.0) - 2.7725887 * jax.random.uniform(streams_of[12], (LAYERS, D, 3 * D), jnp.float32) ** steps_of(streams_of[12], (LAYERS, D, 3 * D), ((0, 4), (1, 8)), -0.2, 0.2)), 0.25, 4.0)
    second_out = jnp.clip(jnp.exp(math.log(4.0) - 2.7725887 * jax.random.uniform(streams_of[13], (LAYERS, D, D), jnp.float32) ** steps_of(streams_of[13], (LAYERS, D, D), ((0, 4), (1, 8)), -0.2, 0.2)), 0.25, 4.0)
    return {"latents": latents, "noise": noise, "timesteps": timesteps, "cameras": cameras, "embed_in": embed_in, "camera_table": camera_table, "w_mod": w_mod, "w_qkv": w_qkv, "w_out": w_out, "head_out": head_out, "moment_qkv": moment_qkv, "moment_out": moment_out, "second_qkv": second_qkv, "second_out": second_out}


def time_embed(step_ids, emb_width):
    half_dim = emb_width // 2
    frequency = jnp.exp(-math.log(10000.0) * jnp.arange(half_dim, dtype=jnp.float32) / half_dim)
    phases = step_ids.astype(jnp.float32)[:, None] * frequency[None, :]
    joined = jnp.concatenate([jnp.cos(phases), jnp.sin(phases)], axis=-1)
    return jax.nn.silu(joined).astype(jnp.bfloat16)

def embed_sample(latent_now, noise_now, step_now, camera_now, embed_in, camera_table):
    step_f = step_now.astype(jnp.float32)
    alpha_bar = jnp.cos((step_f / 1000.0 + 0.008) / 1.008 * (math.pi / 2.0)) ** 2
    noised = jnp.sqrt(alpha_bar) * latent_now.astype(jnp.float32) + jnp.sqrt(1.0 - alpha_bar) * noise_now.astype(jnp.float32)
    features = lax.dot_general(noised.astype(jnp.bfloat16), embed_in, (((0,), (0,)), ((), ())), preferred_element_type=jnp.float32)
    onehot = (camera_now[:, None] == jnp.arange(camera_table.shape[0], dtype=jnp.int32)[None, :]).astype(jnp.bfloat16)
    camera_vec = jnp.dot(onehot, camera_table, preferred_element_type=jnp.float32)
    model_width = embed_in.shape[1]
    views = camera_now.shape[0]
    joined = features.reshape(views, -1, model_width) + camera_vec[:, None, :]
    return joined.reshape(-1, model_width).astype(jnp.bfloat16)

def normed_of(layer_h, shift_mod, scale_mod):
    hidden_f = layer_h.astype(jnp.float32)
    mean_sq = lax.optimization_barrier(jnp.mean(hidden_f * hidden_f, axis=-1, keepdims=True))
    return (hidden_f * lax.rsqrt(mean_sq + 1e-06) * (1.0 + scale_mod) + shift_mod).astype(jnp.bfloat16)

def piece_a(layer_h, weight_qkv, shift_mod, scale_mod):
    normed = normed_of(layer_h, shift_mod, scale_mod)
    return jnp.dot(normed, weight_qkv, preferred_element_type=jnp.float32).astype(jnp.bfloat16)

def piece_b(qkv_rows):
    seq_len = qkv_rows.shape[0]
    model_width = qkv_rows.shape[1] // 3
    queries = qkv_rows[:, :model_width].reshape(seq_len, HEADS, HEAD_DIM).astype(jnp.float32)
    keys_in = qkv_rows[:, model_width:2 * model_width].reshape(seq_len, HEADS, HEAD_DIM).astype(jnp.float32)
    values_in = qkv_rows[:, 2 * model_width:].reshape(seq_len, HEADS, HEAD_DIM).astype(jnp.float32)
    scores = jnp.einsum('qhd,khd->hqk', queries, keys_in) * (1.0 / math.sqrt(HEAD_DIM))
    probabilities = jax.nn.softmax(scores, axis=-1).astype(jnp.bfloat16)
    attended = jnp.einsum('hqk,khd->qhd', probabilities.astype(jnp.float32), values_in)
    return attended.reshape(seq_len, model_width).astype(jnp.bfloat16)

def piece_c(attended, layer_h, weight_out, gate_mod):
    projected = jnp.dot(attended, weight_out, preferred_element_type=jnp.float32)
    return (layer_h.astype(jnp.float32) + gate_mod * projected).astype(jnp.bfloat16)

def output_grad(final_h, head_out, noise_now):

    def squared(hidden_in):
        hidden_f = hidden_in.astype(jnp.float32)
        mean_sq = lax.optimization_barrier(jnp.mean(hidden_f * hidden_f, axis=-1, keepdims=True))
        normed = (hidden_f * lax.rsqrt(mean_sq + 1e-06)).astype(jnp.bfloat16)
        predicted = lax.dot_general(head_out, normed, (((1,), (1,)), ((), ())), preferred_element_type=jnp.float32)
        error_val = predicted - noise_now.astype(jnp.float32)
        return jnp.sum(error_val * error_val)
    loss_val, pull_back = jax.vjp(squared, final_h)
    return pull_back(jnp.ones_like(loss_val))[0]

def layer_backward(grad_out, layer_h, qkv_rows, attended, weight_qkv, weight_out, shift_mod, scale_mod, gate_mod):
    _, pull_c = jax.vjp(lambda attn_in, hidden_in: piece_c(attn_in, hidden_in, weight_out, gate_mod), attended, layer_h)
    grad_attn, grad_res = pull_c(grad_out)
    proj_cot = (gate_mod * grad_out.astype(jnp.float32)).astype(jnp.bfloat16)
    grad_wout = lax.dot_general(attended, proj_cot, (((0,), (0,)), ((), ())), preferred_element_type=jnp.float32)
    _, pull_b = jax.vjp(piece_b, qkv_rows)
    grad_qkv_rows = pull_b(grad_attn)[0]
    _, pull_a = jax.vjp(lambda hidden_in: piece_a(hidden_in, weight_qkv, shift_mod, scale_mod), layer_h)
    grad_hidden = pull_a(grad_qkv_rows)[0]
    normed = normed_of(layer_h, shift_mod, scale_mod)
    grad_wqkv = lax.dot_general(normed, grad_qkv_rows, (((0,), (0,)), ((), ())), preferred_element_type=jnp.float32)
    grad_total = (grad_hidden.astype(jnp.float32) + grad_res.astype(jnp.float32)).astype(jnp.bfloat16)
    return (grad_total, grad_wqkv, grad_wout)

def optimizer_step(gradient, moment, second, factor):
    normalized = gradient * factor
    moment_new = 0.9 * moment + 0.1 * normalized
    second_new = 0.99 * second + 0.01 * normalized * normalized
    return (moment_new / (jnp.sqrt(second_new) + 1e-08), moment_new, second_new)

def reference(latents, noise, timesteps, cameras, embed_in, camera_table, w_mod, w_qkv, w_out, head_out, moment_qkv, moment_out, second_qkv, second_out):
    model_width = w_qkv.shape[1]
    time_emb = time_embed(timesteps, w_mod.shape[1])

    def per_sample(carried, sample_item):
        latent_now, noise_now, emb_now, camera_now, step_now = sample_item
        layer_h = embed_sample(latent_now, noise_now, step_now, camera_now, embed_in, camera_table)
        stored = []
        for layer_num in range(LAYERS):
            modulation = jnp.dot(emb_now[None, :], w_mod[layer_num], preferred_element_type=jnp.float32)[0]
            shift_mod = modulation[:model_width]
            scale_mod = modulation[model_width:2 * model_width]
            gate_mod = modulation[2 * model_width:]
            qkv_rows = piece_a(layer_h, w_qkv[layer_num], shift_mod, scale_mod)
            attended = piece_b(qkv_rows)
            stored.append((layer_h, qkv_rows, attended, shift_mod, scale_mod, gate_mod))
            layer_h = piece_c(attended, layer_h, w_out[layer_num], gate_mod)
        grad_h = output_grad(layer_h, head_out, noise_now)
        grads_qkv = [None] * LAYERS
        grads_out = [None] * LAYERS
        for layer_num in reversed(range(LAYERS)):
            saved_h, qkv_rows, attended, shift_mod, scale_mod, gate_mod = stored[layer_num]
            grad_h, grads_qkv[layer_num], grads_out[layer_num] = layer_backward(grad_h, saved_h, qkv_rows, attended, w_qkv[layer_num], w_out[layer_num], shift_mod, scale_mod, gate_mod)
        return ((carried[0] + jnp.stack(grads_qkv), carried[1] + jnp.stack(grads_out)), None)
    start = (jnp.zeros(w_qkv.shape, jnp.float32), jnp.zeros(w_out.shape, jnp.float32))
    (grad_qkv, grad_out), _ = lax.scan(per_sample, start, (latents, noise, time_emb, cameras, timesteps))
    total_sq = jnp.sum(grad_qkv * grad_qkv) + jnp.sum(grad_out * grad_out)
    factor = lax.rsqrt(total_sq / (LAYERS * 4 * model_width * model_width) + 1e-12)
    update_qkv, new_moment_qkv, new_second_qkv = optimizer_step(grad_qkv, moment_qkv, second_qkv, factor)
    update_out, new_moment_out, new_second_out = optimizer_step(grad_out, moment_out, second_out, factor)
    return (update_qkv, update_out, new_moment_qkv, new_moment_out, new_second_qkv, new_second_out)
```

```python
import functools
import math

import jax
import jax.numpy as jnp
from jax import lax
from jax.experimental import pallas as pl
from jax.experimental.pallas import tpu as pltpu
from jax.sharding import PartitionSpec as P

HEADS = 16
HEAD_DIM = 64


def time_embed(step_ids, emb_width):
    half_dim = emb_width // 2
    frequency = jnp.exp(-math.log(10000.0) * jnp.arange(half_dim, dtype=jnp.float32) / half_dim)
    phases = step_ids.astype(jnp.float32)[:, None] * frequency[None, :]
    joined = jnp.concatenate([jnp.cos(phases), jnp.sin(phases)], axis=-1)
    return jax.nn.silu(joined).astype(jnp.bfloat16)


def embed_sample(latent_now, noise_now, step_now, camera_now, embed_in, camera_table):
    step_f = step_now.astype(jnp.float32)
    alpha_bar = jnp.cos((step_f / 1000.0 + 0.008) / 1.008 * (math.pi / 2.0)) ** 2
    noised = jnp.sqrt(alpha_bar) * latent_now.astype(jnp.float32) + jnp.sqrt(
        1.0 - alpha_bar
    ) * noise_now.astype(jnp.float32)
    features = lax.dot_general(
        noised.astype(jnp.bfloat16),
        embed_in,
        (((0,), (0,)), ((), ())),
        preferred_element_type=jnp.float32,
    )
    onehot = (
        camera_now[:, None] == jnp.arange(camera_table.shape[0], dtype=jnp.int32)[None, :]
    ).astype(jnp.bfloat16)
    camera_vec = jnp.dot(onehot, camera_table, preferred_element_type=jnp.float32)
    model_width = embed_in.shape[1]
    views = camera_now.shape[0]
    joined = features.reshape(views, -1, model_width) + camera_vec[:, None, :]
    return joined.reshape(-1, model_width).astype(jnp.bfloat16)


MESH = pl.DeviceIdType.MESH
F32 = jnp.float32
BF16 = jnp.bfloat16
NT = (((1,), (1,)), ((), ()))


def dot(a, b):
    return jnp.dot(a, b, preferred_element_type=F32)


def dot_nt(a, b):
    return lax.dot_general(a, b, NT, preferred_element_type=F32)


def lane_masks():
    lane = lax.broadcasted_iota(jnp.int32, (1, 2 * HEAD_DIM), 1)
    low = jnp.where(lane < HEAD_DIM, 1.0, 0.0)
    return low.astype(BF16), (1.0 - low).astype(BF16)


def stacked(x, masks):
    return jnp.concatenate([x * masks[0], x * masks[1]], axis=0)


def step_kernel(
    h0_ref, mod_ref, noise_ref, head_ref, wqkv_hbm, wout_hbm,
    gqkv_ref, gout_ref, total_ref,
    wqkv, wout, h_in, h_recv, h_out, g_recv, g_send, nrm, qkv, att, datt, probs,
    n_own, a_own, n_par, a_par, c_own, c_par, z_send, z_recv,
    sq_own, sq_recv, sq_mid, sq_sec,
    w_sem, fwd_sem, bwd_sem, t_sem, c_sem, zs_sem, zr_sem, qs_sem, qr_sem, ss_sem, sr_sem,
):
    sections = lax.axis_size("section")
    ranks = lax.axis_size("dp")
    sec = lax.axis_index("section")
    me = lax.axis_index("dp")
    partner = me + 1 - 2 * lax.rem(me, 2)
    half = ranks // 2
    rows, width = h_in.shape
    micro = mod_ref.shape[0]
    seq = rows // micro
    share = width // ranks
    pairs = width // (2 * HEAD_DIM)

    load_qkv = pltpu.make_async_copy(wqkv_hbm, wqkv, w_sem.at[0])
    load_out = pltpu.make_async_copy(wout_hbm, wout, w_sem.at[1])
    load_qkv.start()
    load_out.start()

    barrier = pltpu.get_barrier_semaphore()

    def greet_rank(o, carry):
        pl.semaphore_signal(
            barrier, inc=1, device_id={"dp": lax.rem(me + o, ranks)}, device_id_type=MESH
        )
        return carry

    def greet_section(o, carry):
        pl.semaphore_signal(
            barrier, inc=1, device_id={"section": lax.rem(sec + o, sections)}, device_id_type=MESH
        )
        return carry

    lax.fori_loop(1, ranks, greet_rank, 0)
    lax.fori_loop(1, sections, greet_section, 0)
    pl.semaphore_wait(barrier, ranks - 1 + sections - 1)

    def remote(src, dst, send, recv, device):
        return pltpu.make_async_remote_copy(
            src_ref=src, dst_ref=dst, send_sem=send, recv_sem=recv,
            device_id=device, device_id_type=MESH,
        )

    forward = remote(
        h_out, h_recv, fwd_sem.at[0], fwd_sem.at[1],
        {"section": jnp.minimum(sec + 1, sections - 1)},
    )
    back = remote(
        g_send, g_recv, bwd_sem.at[0], bwd_sem.at[1], {"section": jnp.maximum(sec - 1, 0)}
    )
    swap_n = remote(n_own, n_par, t_sem.at[0], t_sem.at[1], {"dp": partner})
    swap_a = remote(a_own, a_par, t_sem.at[2], t_sem.at[3], {"dp": partner})
    swap_c = [
        remote(c_own.at[b], c_par.at[b], c_sem.at[0, b], c_sem.at[1, b], {"dp": partner})
        for b in range(4)
    ]

    def sample(s):
        return pl.ds(s * seq, seq)

    def mod_part(s, part):
        return mod_ref[pl.ds(s, 1), pl.ds(part * width, width)]

    @pl.when(sec == 0)
    def _():
        h_in[...] = h0_ref[...]

    @pl.when(sec > 0)
    def _():
        forward.wait_recv()
        h_in[...] = h_recv[...]

    for s in range(micro):
        h = h_in[sample(s), :].astype(F32)
        mean_sq = jnp.mean(h * h, axis=-1, keepdims=True)
        nrm[sample(s), :] = (
            h * lax.rsqrt(mean_sq + 1e-06) * (1.0 + mod_part(s, 1)) + mod_part(s, 0)
        ).astype(BF16)
    load_qkv.wait()
    tile = width // 2

    def qkv_tile(t, carry):
        cols = pl.ds(pl.multiple_of(t * tile, tile), tile)
        qkv[:, cols] = dot(nrm[...], wqkv[:, cols]).astype(BF16)
        return carry

    lax.fori_loop(0, 3 * width // tile, qkv_tile, 0)

    def heads_at(j, part):
        start = part * width + j * 2 * HEAD_DIM
        return pl.ds(pl.multiple_of(start, 2 * HEAD_DIM), 2 * HEAD_DIM)

    def attend(j, carry):
        masks = lane_masks()
        for s in range(micro):
            q2 = stacked(qkv[sample(s), heads_at(j, 0)], masks)
            k = qkv[sample(s), heads_at(j, 1)]
            v2 = stacked(qkv[sample(s), heads_at(j, 2)], masks)
            scores = dot_nt(q2, k) * (1.0 / math.sqrt(HEAD_DIM))
            e = jnp.exp(scores - jnp.max(scores, axis=-1, keepdims=True))
            p = e / jnp.sum(e, axis=-1, keepdims=True)
            probs[s * pairs + j] = p
            p2 = p.astype(BF16)
            wide = jnp.concatenate([p2[:seq], p2[seq:]], axis=1)
            att[sample(s), heads_at(j, 0)] = dot(wide, v2).astype(BF16)
        return carry

    lax.fori_loop(0, pairs, attend, 0, unroll=2)
    load_out.wait()
    otile = width // 4

    def out_tile(t, carry):
        cols = pl.ds(pl.multiple_of(t * otile, otile), otile)
        projected = dot(att[...], wout[:, cols])
        for s in range(micro):
            gate = mod_ref[pl.ds(s, 1), pl.ds(pl.multiple_of(2 * width + t * otile, otile), otile)]
            h = h_in[sample(s), cols].astype(F32)
            h_out[sample(s), cols] = (
                h + gate * projected[s * seq : (s + 1) * seq]
            ).astype(BF16)
        return carry

    lax.fori_loop(0, width // otile, out_tile, 0)

    @pl.when(sec < sections - 1)
    def _():
        forward.start()

    def turn(t, carry):
        cols = pl.ds(pl.multiple_of(t * otile, otile), otile)
        n_own[cols, :] = nrm[:, cols].T
        a_own[cols, :] = att[:, cols].T
        return carry

    lax.fori_loop(0, width // otile, turn, 0)
    swap_n.start()
    swap_a.start()

    @pl.when(sec == sections - 1)
    def _():
        for s in range(micro):
            h = h_out[sample(s), :].astype(F32)
            r = lax.rsqrt(jnp.mean(h * h, axis=-1, keepdims=True) + 1e-06)
            n = (h * r).astype(BF16)
            predicted = dot_nt(head_ref[...], n)
            err = 2.0 * (predicted - noise_ref[s])
            dn = dot(err.T.astype(BF16), head_ref[...]).astype(BF16).astype(F32)
            dh = r * dn - h * (r * r * r) * jnp.mean(dn * h, axis=-1, keepdims=True)
            g_recv[sample(s), :] = dh.astype(BF16)

    @pl.when(sec < sections - 1)
    def _():
        back.wait_recv()

    for s in range(micro):
        c_own[0, sample(s), :] = (
            mod_part(s, 2) * g_recv[sample(s), :].astype(F32)
        ).astype(BF16)
    swap_c[0].start()

    def datt_tile(t, carry):
        cols = pl.ds(pl.multiple_of(t * otile, otile), otile)
        datt[:, cols] = dot_nt(c_own[0], wout[cols, :]).astype(BF16)
        return carry

    lax.fori_loop(0, width // otile, datt_tile, 0)

    def attend_back(j, carry):
        masks = lane_masks()
        for s in range(micro):
            q2 = stacked(qkv[sample(s), heads_at(j, 0)], masks)
            k2 = stacked(qkv[sample(s), heads_at(j, 1)], masks)
            v = qkv[sample(s), heads_at(j, 2)]
            da2 = stacked(datt[sample(s), heads_at(j, 0)], masks)
            p = probs[s * pairs + j]
            dp = dot_nt(da2, v).astype(BF16).astype(F32)
            ds = (p * (dp - jnp.sum(dp * p, axis=-1, keepdims=True))) * (
                1.0 / math.sqrt(HEAD_DIM)
            )
            db = ds.astype(BF16)
            wide = jnp.concatenate([db[:seq], db[seq:]], axis=1)
            c_own[1, sample(s), heads_at(j, 0)] = dot(wide, k2).astype(BF16)
            c_own[2, sample(s), heads_at(j, 0)] = dot(ds.T.astype(BF16), q2).astype(BF16)
            c_own[3, sample(s), heads_at(j, 0)] = dot(p.T.astype(BF16), da2).astype(BF16)
        return carry

    lax.fori_loop(0, pairs, attend_back, 0, unroll=2)
    for b in range(1, 4):
        swap_c[b].start()

    @pl.when(sec > 0)
    def _():
        def dn_tile(t, carry):
            cols = pl.ds(pl.multiple_of(t * otile, otile), otile)
            datt[:, cols] = (
                dot_nt(c_own[1], wqkv[cols, pl.ds(0, width)])
                + dot_nt(c_own[2], wqkv[cols, pl.ds(width, width)])
                + dot_nt(c_own[3], wqkv[cols, pl.ds(2 * width, width)])
            ).astype(BF16)
            return carry

        lax.fori_loop(0, width // otile, dn_tile, 0)
        for s in range(micro):
            h = h_in[sample(s), :].astype(F32)
            r = lax.rsqrt(jnp.mean(h * h, axis=-1, keepdims=True) + 1e-06)
            g = datt[sample(s), :].astype(F32) * (1.0 + mod_part(s, 1))
            dh = r * g - h * (r * r * r) * jnp.mean(g * h, axis=-1, keepdims=True)
            g_send[sample(s), :] = (
                dh.astype(BF16).astype(F32) + g_recv[sample(s), :].astype(F32)
            ).astype(BF16)
        back.start()

    swap_a.wait()
    swap_n.wait()

    def chunk_of(b, rank):
        at = pl.ds(pl.multiple_of(rank * share, share), share)
        own, par = (a_own, a_par) if b == 0 else (n_own, n_par)
        return dot(own[at, :], c_own[b]) + dot(par[at, :], c_par[b])

    def copy_z(b, o):
        return remote(
            z_send.at[b, o - 1], z_recv.at[b, o - 1], zs_sem.at[b, o - 1], zr_sem.at[b, o - 1],
            {"dp": lax.rem(me + 2 * o, ranks)},
        )

    for b in range(4):
        swap_c[b].wait()

        def send_chunk(o, carry, b=b):
            z_send[b, o - 1] = chunk_of(b, lax.rem(me + 2 * o, ranks)).astype(BF16)
            copy_z(b, o).start()
            return carry

        lax.fori_loop(1, half, send_chunk, 0)
    square = jnp.zeros((share, width), F32)
    for b in range(4):
        mine = chunk_of(b, me)

        if b == 0:
            gout_ref[...] = mine
        else:
            gqkv_ref[:, pl.ds((b - 1) * width, width)] = mine
    for b in range(4):
        target = gout_ref if b == 0 else gqkv_ref.at[:, pl.ds((b - 1) * width, width)]

        def add_in(o, carry, b=b, target=target):
            copy_z(b, o).wait()
            target[...] += z_recv[b, o - 1].astype(F32)
            return carry

        lax.fori_loop(1, half, add_in, 0)
        square = square + target[...] * target[...]
    row = jnp.sum(square, axis=0, keepdims=True)
    part = row[:, :128]
    for c in range(1, width // 128):
        part = part + row[:, c * 128 : (c + 1) * 128]
    sq_own[...] = jnp.broadcast_to(part, sq_own.shape)

    def copy_q(o):
        return remote(
            sq_own, sq_recv.at[o - 1], qs_sem.at[o - 1], qr_sem.at[o - 1],
            {"dp": lax.rem(me + o, ranks)},
        )

    def copy_s(o):
        return remote(
            sq_mid, sq_sec.at[o - 1], ss_sem.at[o - 1], sr_sem.at[o - 1],
            {"section": lax.rem(sec + o, sections)},
        )

    def start_with(make):
        def go(o, carry):
            make(o).start()
            return carry

        return go

    def sum_with(make, landed):
        def go(o, total):
            make(o).wait()
            return total + landed[o - 1]

        return go

    lax.fori_loop(1, ranks, start_with(copy_q), 0)
    sq_mid[...] = lax.fori_loop(1, ranks, sum_with(copy_q, sq_recv), sq_own[...])
    lax.fori_loop(1, sections, start_with(copy_s), 0)
    total_ref[...] = lax.fori_loop(1, sections, sum_with(copy_s, sq_sec), sq_mid[...])

    @pl.when(sec < sections - 1)
    def _():
        forward.wait_send()

    @pl.when(sec > 0)
    def _():
        back.wait_send()


def train_step(h0, modulation, noise_pad, head_pad, w_qkv, w_out, sections, ranks):
    rows, width = h0.shape
    micro = modulation.shape[0]
    seq = rows // micro
    half = ranks // 2
    share = width // ranks
    pairs = width // (2 * HEAD_DIM)
    act = pltpu.VMEM((rows, width), BF16)
    turned = pltpu.VMEM((width, rows), BF16)
    vmem = pl.BlockSpec(memory_space=pltpu.VMEM)
    hbm = pl.BlockSpec(memory_space=pl.ANY)
    dma = pltpu.SemaphoreType.DMA
    return pl.pallas_call(
        step_kernel,
        out_shape=(
            jax.ShapeDtypeStruct((share, 3 * width), F32),
            jax.ShapeDtypeStruct((share, width), F32),
            jax.ShapeDtypeStruct((8, 128), F32),
        ),
        in_specs=[vmem, vmem, vmem, vmem, hbm, hbm],
        out_specs=(vmem, vmem, vmem),
        scratch_shapes=[
            pltpu.VMEM(w_qkv.shape, BF16),
            pltpu.VMEM(w_out.shape, BF16),
            act, act, act, act, act, act,
            pltpu.VMEM((rows, 3 * width), BF16),
            act, act,
            pltpu.VMEM((micro * pairs, 2 * seq, seq), F32),
            turned, turned, turned, turned,
            pltpu.VMEM((4, rows, width), BF16),
            pltpu.VMEM((4, rows, width), BF16),
            pltpu.VMEM((4, half - 1, share, width), BF16),
            pltpu.VMEM((4, half - 1, share, width), BF16),
            pltpu.VMEM((8, 128), F32),
            pltpu.VMEM((ranks - 1, 8, 128), F32),
            pltpu.VMEM((8, 128), F32),
            pltpu.VMEM((sections - 1, 8, 128), F32),
            dma((2,)), dma((2,)), dma((2,)), dma((4,)), dma((2, 4)),
            dma((4, half - 1)), dma((4, half - 1)),
            dma((ranks - 1,)), dma((ranks - 1,)),
            dma((sections - 1,)), dma((sections - 1,)),
        ],
        compiler_params=pltpu.CompilerParams(
            collective_id=0, has_side_effects=True, vmem_limit_bytes=60 * 1024 * 1024
        ),
    )(h0, modulation, noise_pad, head_pad, w_qkv, w_out)


def optimizer_step(gradient, moment, second, factor):
    normalized = gradient * factor
    moment_new = 0.9 * moment + 0.1 * normalized
    second_new = 0.99 * second + 0.01 * normalized * normalized
    return (moment_new / (jnp.sqrt(second_new) + 1e-08), moment_new, second_new)


def local(
    latents,
    noise,
    timesteps,
    cameras,
    embed_in,
    camera_table,
    w_mod,
    w_qkv,
    w_out,
    head_out,
    moment_qkv,
    moment_out,
    second_qkv,
    second_out,
):
    sections = lax.axis_size("section")
    ranks = lax.axis_size("dp")
    model_width = w_qkv.shape[1]
    time_emb = time_embed(timesteps, w_mod.shape[1])
    modulation = jnp.dot(time_emb, w_mod[0], preferred_element_type=jnp.float32)
    h0 = jax.vmap(embed_sample, in_axes=(0, 0, 0, 0, None, None))(
        latents, noise, timesteps, cameras, embed_in, camera_table
    ).reshape(-1, model_width)
    channels = noise.shape[1]
    noise_pad = jnp.pad(noise.astype(F32), ((0, 0), (0, 128 - channels), (0, 0)))
    head_pad = jnp.pad(head_out, ((0, 128 - channels), (0, 0)))
    grad_qkv, grad_out, total = train_step(
        h0, modulation, noise_pad, head_pad, w_qkv[0], w_out[0], sections, ranks
    )
    total_sq = jnp.sum(total[0])
    factor = lax.rsqrt(total_sq / (sections * 4 * model_width * model_width) + 1e-12)
    update_qkv, new_moment_qkv, new_second_qkv = optimizer_step(
        grad_qkv[None], moment_qkv, second_qkv, factor
    )
    update_out, new_moment_out, new_second_out = optimizer_step(
        grad_out[None], moment_out, second_out, factor
    )
    return (update_qkv, update_out, new_moment_qkv, new_moment_out, new_second_qkv, new_second_out)


def solution(mesh):
    placed = (
        P("dp", None, None),
        P("dp", None, None),
        P("dp"),
        P("dp", None),
        P(),
        P(),
        P("section", None, None),
        P("section", None, None),
        P("section", None, None),
        P(),
        P("section", "dp", None),
        P("section", "dp", None),
        P("section", "dp", None),
        P("section", "dp", None),
    )
    return jax.shard_map(
        local,
        mesh=mesh,
        in_specs=placed,
        out_specs=(
            P("section", "dp", None),
            P("section", "dp", None),
            P("section", "dp", None),
            P("section", "dp", None),
            P("section", "dp", None),
            P("section", "dp", None),
        ),
        check_vma=False,
    )
```

```python
import functools
import math

import jax
import jax.numpy as jnp
from jax import lax
from jax.experimental import pallas as pl
from jax.experimental.pallas import tpu as pltpu
from jax.sharding import PartitionSpec as P

HEADS = 16
HEAD_DIM = 64


def time_embed(step_ids, emb_width):
    half_dim = emb_width // 2
    frequency = jnp.exp(-math.log(10000.0) * jnp.arange(half_dim, dtype=jnp.float32) / half_dim)
    phases = step_ids.astype(jnp.float32)[:, None] * frequency[None, :]
    joined = jnp.concatenate([jnp.cos(phases), jnp.sin(phases)], axis=-1)
    return jax.nn.silu(joined).astype(jnp.bfloat16)


def embed_sample(latent_now, noise_now, step_now, camera_now, embed_in, camera_table):
    step_f = step_now.astype(jnp.float32)
    alpha_bar = jnp.cos((step_f / 1000.0 + 0.008) / 1.008 * (math.pi / 2.0)) ** 2
    noised = jnp.sqrt(alpha_bar) * latent_now.astype(jnp.float32) + jnp.sqrt(
        1.0 - alpha_bar
    ) * noise_now.astype(jnp.float32)
    features = lax.dot_general(
        noised.astype(jnp.bfloat16),
        embed_in,
        (((0,), (0,)), ((), ())),
        preferred_element_type=jnp.float32,
    )
    onehot = (
        camera_now[:, None] == jnp.arange(camera_table.shape[0], dtype=jnp.int32)[None, :]
    ).astype(jnp.bfloat16)
    camera_vec = jnp.dot(onehot, camera_table, preferred_element_type=jnp.float32)
    model_width = embed_in.shape[1]
    views = camera_now.shape[0]
    joined = features.reshape(views, -1, model_width) + camera_vec[:, None, :]
    return joined.reshape(-1, model_width).astype(jnp.bfloat16)


MESH = pl.DeviceIdType.MESH
F32 = jnp.float32
BF16 = jnp.bfloat16
NT = (((1,), (1,)), ((), ()))


def dot(a, b):
    return jnp.dot(a, b, preferred_element_type=F32)


def dot_nt(a, b):
    return lax.dot_general(a, b, NT, preferred_element_type=F32)


def lane_masks():
    lane = lax.broadcasted_iota(jnp.int32, (1, 2 * HEAD_DIM), 1)
    low = jnp.where(lane < HEAD_DIM, 1.0, 0.0)
    return low.astype(BF16), (1.0 - low).astype(BF16)


def stacked(x, masks):
    return jnp.concatenate([x * masks[0], x * masks[1]], axis=0)


def step_kernel(
    h0_ref, mod_ref, noise_ref, head_ref, wqkv_hbm, wout_hbm,
    gqkv_ref, gout_ref, total_ref,
    wqkv, wout, h_in, h_recv, h_out, g_recv, g_send, nrm, qkv, att, datt, probs,
    n_own, a_own, n_par, a_par, c_own, c_par, z_send, z_recv,
    sq_own, sq_recv, sq_mid, sq_sec,
    w_sem, fwd_sem, bwd_sem, t_sem, c_sem, zs_sem, zr_sem, qs_sem, qr_sem, ss_sem, sr_sem,
):
    sections = lax.axis_size("section")
    ranks = lax.axis_size("dp")
    sec = lax.axis_index("section")
    me = lax.axis_index("dp")
    partner = me + 1 - 2 * lax.rem(me, 2)
    half = ranks // 2
    rows, width = h_in.shape
    micro = mod_ref.shape[0]
    seq = rows // micro
    share = width // ranks
    pairs = width // (2 * HEAD_DIM)

    load_qkv = pltpu.make_async_copy(wqkv_hbm, wqkv, w_sem.at[0])
    load_out = pltpu.make_async_copy(wout_hbm, wout, w_sem.at[1])
    load_qkv.start()
    load_out.start()

    barrier = pltpu.get_barrier_semaphore()

    def greet_rank(o, carry):
        pl.semaphore_signal(
            barrier, inc=1, device_id={"dp": lax.rem(me + o, ranks)}, device_id_type=MESH
        )
        return carry

    def greet_section(o, carry):
        pl.semaphore_signal(
            barrier, inc=1, device_id={"section": lax.rem(sec + o, sections)}, device_id_type=MESH
        )
        return carry

    lax.fori_loop(1, ranks, greet_rank, 0)
    lax.fori_loop(1, sections, greet_section, 0)
    pl.semaphore_wait(barrier, ranks - 1 + sections - 1)

    def remote(src, dst, send, recv, device):
        return pltpu.make_async_remote_copy(
            src_ref=src, dst_ref=dst, send_sem=send, recv_sem=recv,
            device_id=device, device_id_type=MESH,
        )

    def forward(s):
        at = pl.ds(s * seq, seq)
        return remote(
            h_out.at[at], h_recv.at[at], fwd_sem.at[0, s], fwd_sem.at[1, s],
            {"section": jnp.minimum(sec + 1, sections - 1)},
        )

    def back(s):
        at = pl.ds(s * seq, seq)
        return remote(
            g_send.at[at], g_recv.at[at], bwd_sem.at[0, s], bwd_sem.at[1, s],
            {"section": jnp.maximum(sec - 1, 0)},
        )

    swap_n = remote(n_own, n_par, t_sem.at[0], t_sem.at[1], {"dp": partner})
    swap_a = remote(a_own, a_par, t_sem.at[2], t_sem.at[3], {"dp": partner})
    def swap_c(b, s):
        at = pl.ds(s * seq, seq)
        return remote(
            c_own.at[b, at], c_par.at[b, at], c_sem.at[0, b, s], c_sem.at[1, b, s],
            {"dp": partner},
        )

    def sample(s):
        return pl.ds(s * seq, seq)

    def mod_part(s, part):
        return mod_ref[pl.ds(s, 1), pl.ds(part * width, width)]

    tile = width // 2
    otile = width // 4

    def heads_at(j, part):
        start = part * width + j * 2 * HEAD_DIM
        return pl.ds(pl.multiple_of(start, 2 * HEAD_DIM), 2 * HEAD_DIM)

    def layer_forward(s):
        here = sample(s)

        @pl.when(sec == 0)
        def _():
            h_in[here, :] = h0_ref[here, :]

        @pl.when(sec > 0)
        def _():
            forward(s).wait_recv()
            h_in[here, :] = h_recv[here, :]

        h = h_in[here, :].astype(F32)
        mean_sq = jnp.mean(h * h, axis=-1, keepdims=True)
        nrm[here, :] = (
            h * lax.rsqrt(mean_sq + 1e-06) * (1.0 + mod_part(s, 1)) + mod_part(s, 0)
        ).astype(BF16)
        if s == 0:
            load_qkv.wait()

        def qkv_tile(t, carry):
            cols = pl.ds(pl.multiple_of(t * tile, tile), tile)
            qkv[here, cols] = dot(nrm[here, :], wqkv[:, cols]).astype(BF16)
            return carry

        lax.fori_loop(0, 3 * width // tile, qkv_tile, 0)

        def attend(j, carry):
            masks = lane_masks()
            q2 = stacked(qkv[here, heads_at(j, 0)], masks)
            k = qkv[here, heads_at(j, 1)]
            v2 = stacked(qkv[here, heads_at(j, 2)], masks)
            scores = dot_nt(q2, k) * (1.0 / math.sqrt(HEAD_DIM))
            e = jnp.exp(scores - jnp.max(scores, axis=-1, keepdims=True))
            p = e / jnp.sum(e, axis=-1, keepdims=True)
            probs[s * pairs + j] = p
            p2 = p.astype(BF16)
            wide = jnp.concatenate([p2[:seq], p2[seq:]], axis=1)
            att[here, heads_at(j, 0)] = dot(wide, v2).astype(BF16)
            return carry

        lax.fori_loop(0, pairs, attend, 0, unroll=4)
        if s == 0:
            load_out.wait()

        def out_tile(t, carry):
            cols = pl.ds(pl.multiple_of(t * otile, otile), otile)
            gate = mod_ref[pl.ds(s, 1), pl.ds(pl.multiple_of(2 * width + t * otile, otile), otile)]
            h_out[here, cols] = (
                h_in[here, cols].astype(F32) + gate * dot(att[here, :], wout[:, cols])
            ).astype(BF16)
            return carry

        lax.fori_loop(0, width // otile, out_tile, 0)

        @pl.when(sec < sections - 1)
        def _():
            forward(s).start()

    def swap_turned():
        def turn(t, carry):
            cols = pl.ds(pl.multiple_of(t * otile, otile), otile)
            n_own[cols, :] = nrm[:, cols].T
            a_own[cols, :] = att[:, cols].T
            return carry

        lax.fori_loop(0, width // otile, turn, 0)
        swap_n.start()
        swap_a.start()

    def layer_backward(s):
        here = sample(s)

        @pl.when(sec == sections - 1)
        def _():
            h = h_out[here, :].astype(F32)
            r = lax.rsqrt(jnp.mean(h * h, axis=-1, keepdims=True) + 1e-06)
            n = (h * r).astype(BF16)
            predicted = dot_nt(head_ref[...], n)
            err = 2.0 * (predicted - noise_ref[s])
            dn = dot(err.T.astype(BF16), head_ref[...]).astype(BF16).astype(F32)
            dh = r * dn - h * (r * r * r) * jnp.mean(dn * h, axis=-1, keepdims=True)
            g_recv[here, :] = dh.astype(BF16)

        @pl.when(sec < sections - 1)
        def _():
            back(s).wait_recv()

        c_own[0, here, :] = (mod_part(s, 2) * g_recv[here, :].astype(F32)).astype(BF16)

        def datt_tile(t, carry):
            cols = pl.ds(pl.multiple_of(t * otile, otile), otile)
            datt[here, cols] = dot_nt(c_own[0, here, :], wout[cols, :]).astype(BF16)
            return carry

        lax.fori_loop(0, width // otile, datt_tile, 0)
        swap_c(0, s).start()

        def attend_back(j, carry):
            masks = lane_masks()
            q2 = stacked(qkv[here, heads_at(j, 0)], masks)
            k2 = stacked(qkv[here, heads_at(j, 1)], masks)
            v = qkv[here, heads_at(j, 2)]
            da2 = stacked(datt[here, heads_at(j, 0)], masks)
            p = probs[s * pairs + j]
            dp = dot_nt(da2, v).astype(BF16).astype(F32)
            ds = (p * (dp - jnp.sum(dp * p, axis=-1, keepdims=True))) * (
                1.0 / math.sqrt(HEAD_DIM)
            )
            db = ds.astype(BF16)
            wide = jnp.concatenate([db[:seq], db[seq:]], axis=1)
            c_own[1, here, heads_at(j, 0)] = dot(wide, k2).astype(BF16)
            c_own[2, here, heads_at(j, 0)] = dot(ds.T.astype(BF16), q2).astype(BF16)
            c_own[3, here, heads_at(j, 0)] = dot(p.T.astype(BF16), da2).astype(BF16)
            return carry

        lax.fori_loop(0, pairs, attend_back, 0, unroll=4)
        for b in range(1, 4):
            swap_c(b, s).start()

        @pl.when(sec > 0)
        def _():
            def dn_tile(t, carry):
                cols = pl.ds(pl.multiple_of(t * otile, otile), otile)
                datt[here, cols] = (
                    dot_nt(c_own[1, here, :], wqkv[cols, pl.ds(0, width)])
                    + dot_nt(c_own[2, here, :], wqkv[cols, pl.ds(width, width)])
                    + dot_nt(c_own[3, here, :], wqkv[cols, pl.ds(2 * width, width)])
                ).astype(BF16)
                return carry

            lax.fori_loop(0, width // otile, dn_tile, 0)
            h = h_in[here, :].astype(F32)
            r = lax.rsqrt(jnp.mean(h * h, axis=-1, keepdims=True) + 1e-06)
            g = datt[here, :].astype(F32) * (1.0 + mod_part(s, 1))
            dh = r * g - h * (r * r * r) * jnp.mean(g * h, axis=-1, keepdims=True)
            g_send[here, :] = (
                dh.astype(BF16).astype(F32) + g_recv[here, :].astype(F32)
            ).astype(BF16)
            back(s).start()

    for s in range(micro):
        layer_forward(s)

    @pl.when(sec < sections - 1)
    def _():
        swap_turned()

    for s in range(micro):
        layer_backward(s)

    @pl.when(sec == sections - 1)
    def _():
        swap_turned()

    swap_a.wait()
    swap_n.wait()

    def chunk_of(b, rank):
        at = pl.ds(pl.multiple_of(rank * share, share), share)
        own, par = (a_own, a_par) if b == 0 else (n_own, n_par)
        return dot(own[at, :], c_own[b]) + dot(par[at, :], c_par[b])

    def copy_z(b, o):
        return remote(
            z_send.at[b, o - 1], z_recv.at[b, o - 1], zs_sem.at[b, o - 1], zr_sem.at[b, o - 1],
            {"dp": lax.rem(me + 2 * o, ranks)},
        )

    for b in range(4):
        for s in range(micro):
            swap_c(b, s).wait()

        def send_chunk(o, carry, b=b):
            z_send[b, o - 1] = chunk_of(b, lax.rem(me + 2 * o, ranks)).astype(BF16)
            copy_z(b, o).start()
            return carry

        lax.fori_loop(1, half, send_chunk, 0)
    square = jnp.zeros((share, width), F32)
    for b in range(4):
        mine = chunk_of(b, me)

        if b == 0:
            gout_ref[...] = mine
        else:
            gqkv_ref[:, pl.ds((b - 1) * width, width)] = mine
    for b in range(4):
        target = gout_ref if b == 0 else gqkv_ref.at[:, pl.ds((b - 1) * width, width)]

        def add_in(o, carry, b=b, target=target):
            copy_z(b, o).wait()
            target[...] += z_recv[b, o - 1].astype(F32)
            return carry

        lax.fori_loop(1, half, add_in, 0)
        square = square + target[...] * target[...]
    row = jnp.sum(square, axis=0, keepdims=True)
    part = row[:, :128]
    for c in range(1, width // 128):
        part = part + row[:, c * 128 : (c + 1) * 128]
    sq_own[...] = jnp.broadcast_to(part, sq_own.shape)

    def copy_q(o):
        return remote(
            sq_own, sq_recv.at[o - 1], qs_sem.at[o - 1], qr_sem.at[o - 1],
            {"dp": lax.rem(me + o, ranks)},
        )

    def copy_s(o):
        return remote(
            sq_mid, sq_sec.at[o - 1], ss_sem.at[o - 1], sr_sem.at[o - 1],
            {"section": lax.rem(sec + o, sections)},
        )

    def start_with(make):
        def go(o, carry):
            make(o).start()
            return carry

        return go

    def sum_with(make, landed):
        def go(o, total):
            make(o).wait()
            return total + landed[o - 1]

        return go

    lax.fori_loop(1, ranks, start_with(copy_q), 0)
    sq_mid[...] = lax.fori_loop(1, ranks, sum_with(copy_q, sq_recv), sq_own[...])
    lax.fori_loop(1, sections, start_with(copy_s), 0)
    total_ref[...] = lax.fori_loop(1, sections, sum_with(copy_s, sq_sec), sq_mid[...])

    @pl.when(sec < sections - 1)
    def _():
        for s in range(micro):
            forward(s).wait_send()

    @pl.when(sec > 0)
    def _():
        for s in range(micro):
            back(s).wait_send()


def train_step(h0, modulation, noise_pad, head_pad, w_qkv, w_out, sections, ranks):
    rows, width = h0.shape
    micro = modulation.shape[0]
    seq = rows // micro
    half = ranks // 2
    share = width // ranks
    pairs = width // (2 * HEAD_DIM)
    act = pltpu.VMEM((rows, width), BF16)
    turned = pltpu.VMEM((width, rows), BF16)
    vmem = pl.BlockSpec(memory_space=pltpu.VMEM)
    hbm = pl.BlockSpec(memory_space=pl.ANY)
    dma = pltpu.SemaphoreType.DMA
    return pl.pallas_call(
        step_kernel,
        out_shape=(
            jax.ShapeDtypeStruct((share, 3 * width), F32),
            jax.ShapeDtypeStruct((share, width), F32),
            jax.ShapeDtypeStruct((8, 128), F32),
        ),
        in_specs=[vmem, vmem, vmem, vmem, hbm, hbm],
        out_specs=(vmem, vmem, vmem),
        scratch_shapes=[
            pltpu.VMEM(w_qkv.shape, BF16),
            pltpu.VMEM(w_out.shape, BF16),
            act, act, act, act, act, act,
            pltpu.VMEM((rows, 3 * width), BF16),
            act, act,
            pltpu.VMEM((micro * pairs, 2 * seq, seq), F32),
            turned, turned, turned, turned,
            pltpu.VMEM((4, rows, width), BF16),
            pltpu.VMEM((4, rows, width), BF16),
            pltpu.VMEM((4, half - 1, share, width), BF16),
            pltpu.VMEM((4, half - 1, share, width), BF16),
            pltpu.VMEM((8, 128), F32),
            pltpu.VMEM((ranks - 1, 8, 128), F32),
            pltpu.VMEM((8, 128), F32),
            pltpu.VMEM((sections - 1, 8, 128), F32),
            dma((2,)), dma((2, micro)), dma((2, micro)), dma((4,)), dma((2, 4, micro)),
            dma((4, half - 1)), dma((4, half - 1)),
            dma((ranks - 1,)), dma((ranks - 1,)),
            dma((sections - 1,)), dma((sections - 1,)),
        ],
        compiler_params=pltpu.CompilerParams(
            collective_id=0, has_side_effects=True, vmem_limit_bytes=60 * 1024 * 1024
        ),
    )(h0, modulation, noise_pad, head_pad, w_qkv, w_out)


def optimizer_step(gradient, moment, second, factor):
    normalized = gradient * factor
    moment_new = 0.9 * moment + 0.1 * normalized
    second_new = 0.99 * second + 0.01 * normalized * normalized
    return (moment_new / (jnp.sqrt(second_new) + 1e-08), moment_new, second_new)


def local(
    latents,
    noise,
    timesteps,
    cameras,
    embed_in,
    camera_table,
    w_mod,
    w_qkv,
    w_out,
    head_out,
    moment_qkv,
    moment_out,
    second_qkv,
    second_out,
):
    sections = lax.axis_size("section")
    ranks = lax.axis_size("dp")
    model_width = w_qkv.shape[1]
    time_emb = time_embed(timesteps, w_mod.shape[1])
    modulation = jnp.dot(time_emb, w_mod[0], preferred_element_type=jnp.float32)
    h0 = jax.vmap(embed_sample, in_axes=(0, 0, 0, 0, None, None))(
        latents, noise, timesteps, cameras, embed_in, camera_table
    ).reshape(-1, model_width)
    channels = noise.shape[1]
    noise_pad = jnp.pad(noise.astype(F32), ((0, 0), (0, 128 - channels), (0, 0)))
    head_pad = jnp.pad(head_out, ((0, 128 - channels), (0, 0)))
    grad_qkv, grad_out, total = train_step(
        h0, modulation, noise_pad, head_pad, w_qkv[0], w_out[0], sections, ranks
    )
    total_sq = jnp.sum(total[0])
    factor = lax.rsqrt(total_sq / (sections * 4 * model_width * model_width) + 1e-12)
    update_qkv, new_moment_qkv, new_second_qkv = optimizer_step(
        grad_qkv[None], moment_qkv, second_qkv, factor
    )
    update_out, new_moment_out, new_second_out = optimizer_step(
        grad_out[None], moment_out, second_out, factor
    )
    return (update_qkv, update_out, new_moment_qkv, new_moment_out, new_second_qkv, new_second_out)


def solution(mesh):
    placed = (
        P("dp", None, None),
        P("dp", None, None),
        P("dp"),
        P("dp", None),
        P(),
        P(),
        P("section", None, None),
        P("section", None, None),
        P("section", None, None),
        P(),
        P("section", "dp", None),
        P("section", "dp", None),
        P("section", "dp", None),
        P("section", "dp", None),
    )
    return jax.shard_map(
        local,
        mesh=mesh,
        in_specs=placed,
        out_specs=(
            P("section", "dp", None),
            P("section", "dp", None),
            P("section", "dp", None),
            P("section", "dp", None),
            P("section", "dp", None),
            P("section", "dp", None),
        ),
        check_vma=False,
    )
```
